256 devices in a mesh: gx: 16 (over x, y), gy: 16 (over z, core).
Axes of the slice: x: 4, y: 4, z: 8, core: 2. Of those that a mesh axis runs over, the one named last changes fastest.
Arguments:
- matrix_tiles: float32 [32, 64, 6, 128, 128], P('gx', 'gy'), may hold values from -4 to 4.5, as said below
- tile_codes: int32 [32, 64, 6], P('gx', 'gy'), may hold values from 0 to 8, as said below
- tile_counts: int32 [32, 64], P('gx', 'gy'), may hold values from 1 to 6, as said below
- right_side: float32 [32, 64, 128], P('gx', 'gy'), may hold values from -8 to 8
- initial_guess: float32 [32, 64, 128], P('gx', 'gy'), may hold values from -4 to 4
Outputs:
- solution: float32 [32, 64, 128], P('gx', 'gy')
- residual: float32 [32, 64, 128], P('gx', 'gy')
- hessenberg: float32 [5, 4], replicated
The draws below stay inside these ranges and needn't reach their ends.
Inputs may be any that keep to these rules, and one draw needn't show every extreme that they name: tile_codes of slot 0 is 4 (the block itself); the codes of one block row are distinct. `tile_counts`: every block row has at least one live slot; some block row has all 6 slots live. `matrix_tiles`: slot 0 of each block row has a diagonal of 2 to 4 added to its entries.
All inputs are finite; a program needn't handle non-finite values.
Results may differ from the reference program's by a relative error of at most 0.0012.
Values sent between devices are 32-bit elements; how exact they have to be, the bound alone decides.
A program may use at most 64 MiB of HBM per device.

```python
import jax
import jax.numpy as jnp
from jax import lax

BLK = 128
SLOTS = 6
ITERS = 4
RBX = 2
RBY = 4
BX = 32
BY = 64


def draw_matrix_tiles(key, part):
    first, second = jax.random.split(key, 2)
    shape = (BX, BY, SLOTS, BLK, BLK)
    entries = jax.random.normal(first, shape, jnp.float32)
    tiles = entries * (0.5 / jnp.sqrt(jnp.float32(BLK)))
    diagonal = jax.random.uniform(second, (BX, BY, BLK), jnp.float32, 2.0, 4.0)
    identity = jnp.eye(BLK, dtype=jnp.float32)
    return tiles.at[:, :, 0].add(diagonal[:, :, :, None] * identity)


def draw_tile_codes(key, part):
    scores = jax.random.randint(key, (BX, BY, 8), 0, 1 << 20) * 8 + jnp.arange(8, dtype=jnp.int32)
    ordering = jnp.argsort(scores, axis=-1)
    others = jnp.array([0, 1, 2, 3, 5, 6, 7, 8], jnp.int32)[ordering]
    head = jnp.full((BX, BY, 1), 4, jnp.int32)
    return jnp.concatenate([head, others[:, :, :SLOTS - 1]], axis=-1).astype(jnp.int32)


def draw_tile_counts(key, part):
    first, second, third = jax.random.split(key, 3)
    level = jax.random.randint(first, (BX // RBX, BY // RBY), 2, SLOTS + 1)
    level = jnp.repeat(jnp.repeat(level, RBX, axis=0), RBY, axis=1)
    counts = jnp.minimum(jax.random.randint(second, (BX, BY), 1, SLOTS + 1), level)
    position = jax.random.randint(third, (), 0, BX * BY)
    counts = counts.reshape(-1).at[position].set(SLOTS).reshape(BX, BY)
    return counts.astype(jnp.int32)


def shard_levels(own_key, dims, cuts, low, high):
    def one(dim, shards_of):
        heights = jax.random.uniform(jax.random.fold_in(jax.random.fold_in(own_key, 6), dim), (shards_of,), jnp.float32, low / len(cuts), high / len(cuts))
        return jnp.repeat(jnp.exp(heights), dims[dim] // shards_of).reshape((-1,) + (1,) * (len(dims) - dim - 1))

    factor_of = one(*cuts[0])
    for cut in cuts[1:]:
        factor_of = factor_of * one(*cut)
    return factor_of


def noise(own_key, dims, width, reach, cuts=(), kind=jnp.bfloat16):
    level = shard_levels(own_key, dims, cuts, -0.22, 0.18) if cuts else 1.0
    result = jax.random.normal(own_key, dims, jnp.float32) * width * level
    return jnp.minimum(jnp.maximum(result, -reach), reach).astype(kind)


def setup_inputs(seed: int = 0) -> dict:
    splits = jax.random.split(jax.random.key(seed), 6)
    return {
        "matrix_tiles": draw_matrix_tiles(jax.random.fold_in(splits[5], 71), 0),
        "tile_codes": draw_tile_codes(jax.random.fold_in(splits[5], 71), 0),
        "tile_counts": draw_tile_counts(jax.random.fold_in(splits[5], 71), 0),
        "right_side": noise(splits[3], (BX, BY, BLK), 1.0, 8.0, ((0, 16), (1, 16)), jnp.float32),
        "initial_guess": noise(splits[4], (BX, BY, BLK), 0.5, 4.0, ((0, 16), (1, 16)), jnp.float32),
    }


def nine_blocks(padded, height, breadth):
    return jnp.stack([padded[1 + row_step:1 + row_step + height, 1 + col_step:1 + col_step + breadth] for row_step in (-1, 0, 1) for col_step in (-1, 0, 1)])

def apply_matrix(padded, matrix_tiles, tile_codes, tile_counts):
    height, breadth = (tile_codes.shape[0], tile_codes.shape[1])
    stacked = nine_blocks(padded, height, breadth)
    present = jnp.arange(tile_codes.shape[2], dtype=jnp.int32)[None, None, :] < tile_counts[:, :, None]
    onehot = (tile_codes[:, :, :, None] == jnp.arange(9, dtype=jnp.int32)) & present[:, :, :, None]
    onehot = onehot.astype(jnp.float32)
    picked = jnp.einsum('xysc,cxyk->xysk', onehot, stacked, precision=lax.Precision.HIGHEST)
    return jnp.einsum('xyskl,xysl->xyk', matrix_tiles, picked, precision=lax.Precision.HIGHEST)

def operate(field, matrix_tiles, tile_codes, tile_counts):
    padded = jnp.pad(field, ((1, 1), (1, 1), (0, 0)))
    return apply_matrix(padded, matrix_tiles, tile_codes, tile_counts)

def solve_small(lower, target, steps):
    forward = []
    for row in range(steps):
        total = target[row]
        for column in range(row):
            total = total - lower[row, column] * forward[column]
        forward.append(total / lower[row, row])
    backward = [None] * steps
    for row in reversed(range(steps)):
        total = forward[row]
        for column in range(row + 1, steps):
            total = total - lower[column, row] * backward[column]
        backward[row] = total / lower[row, row]
    return backward

def reference(matrix_tiles, tile_codes, tile_counts, right_side, initial_guess):
    start = right_side - operate(initial_guess, matrix_tiles, tile_codes, tile_counts)
    beta = jnp.sqrt(jnp.sum(start * start))
    basis = [start / beta]
    hessenberg = jnp.zeros((ITERS + 1, ITERS), jnp.float32)
    for column in range(ITERS):
        vector_new = operate(basis[column], matrix_tiles, tile_codes, tile_counts)
        for earlier in range(column + 1):
            inner = jnp.sum(vector_new * basis[earlier])
            hessenberg = hessenberg.at[earlier, column].set(inner)
            vector_new = vector_new - inner * basis[earlier]
        length_new = jnp.sqrt(jnp.sum(vector_new * vector_new))
        hessenberg = hessenberg.at[column + 1, column].set(length_new)
        if column + 1 < ITERS:
            basis.append(vector_new / length_new)
    normal_matrix = jnp.dot(hessenberg.T, hessenberg, precision=lax.Precision.HIGHEST)
    target = beta * hessenberg[0, :]
    lower = jnp.linalg.cholesky(normal_matrix)
    weights = solve_small(lower, target, ITERS)
    solution = initial_guess
    for column in range(ITERS):
        solution = solution + weights[column] * basis[column]
    residual = right_side - operate(solution, matrix_tiles, tile_codes, tile_counts)
    return (solution, residual, hessenberg)
```

```python
import functools

import jax
import jax.numpy as jnp
from jax import lax
from jax.experimental import pallas as pl
from jax.experimental.pallas import tpu as pltpu
from jax.sharding import PartitionSpec as P

ITERS = 4
SLOTS = 6
BLK = 128
RBX = 2
RBY = 4
ROWS = RBX * RBY
SHIFT = 3.0
SCALE = 0.25
PAIRS = [(i, j) for j in range(ITERS + 1) for i in range(j + 1)]
MESH = pl.DeviceIdType.MESH

UP, DOWN, LEFT, RIGHT = (0, 4, -1, 0), (4, 4, 1, 0), (8, 2, 0, -1), (10, 2, 0, 1)
CORNERS = ((12, 1, -1, -1), (13, 1, -1, 1), (14, 1, 1, -1), (15, 1, 1, 1))
SIDES = (UP, DOWN, LEFT, RIGHT, *CORNERS)
GRID_OF = (
    [(0, 1 + j) for j in range(RBY)]
    + [(3, 1 + j) for j in range(RBY)]
    + [(1 + i, 0) for i in range(RBX)]
    + [(1 + i, 5) for i in range(RBX)]
    + [(0, 0), (0, 5), (3, 0), (3, 5)]
)
ZERO_ROW = 24


def kernel(
    nx, ny,
    tiles_hbm, codes, counts, right_hbm, guess_hbm,
    solution_ref, residual_ref, hessenberg_ref,
    tiles, grid, where, sent, landed, basis, guess, right,
    gram_rows, gram, line, sums_x, sums_y,
    tile_sems, load_sems, send_sems, recv_sems, sum_send_sems, sum_recv_sems,
):
    gx, gy = lax.axis_index("gx"), lax.axis_index("gy")

    loads = [
        pltpu.make_async_copy(guess_hbm, guess, load_sems.at[0]),
        pltpu.make_async_copy(right_hbm, right, load_sems.at[1]),
    ]
    loads[0].start()
    loads[1].start()
    order = [(i, j) for j in (1, 2) for i in (0, 1)] + [(i, j) for j in (0, 3) for i in (0, 1)]
    tile_loads = {
        (i, j): pltpu.make_async_copy(tiles_hbm.at[i, j], tiles.at[i, j], tile_sems.at[i * RBY + j])
        for i, j in order
    }
    for at in order:
        tile_loads[at].start()

    zero_line = jnp.zeros((1, BLK), jnp.float32)
    for step in range(ITERS + 1):
        for row in range(16):
            landed[step, row] = zero_line
    grid[ZERO_ROW] = zero_line

    def exists(side):
        _, _, dx, dy = side
        ok = None
        for at, d, n in ((gx, dx, nx), (gy, dy, ny)):
            if d:
                here = at > 0 if d < 0 else at < n - 1
                ok = here if ok is None else jnp.logical_and(ok, here)
        return ok

    barrier = pltpu.get_barrier_semaphore()

    def greet(d, _):
        pl.semaphore_signal(
            barrier, inc=1, device_id={"gx": lax.rem(gx + d, nx), "gy": gy}, device_id_type=MESH
        )
        return 0

    def greet_y(d, _):
        pl.semaphore_signal(
            barrier, inc=1, device_id={"gx": gx, "gy": lax.rem(gy + d, ny)}, device_id_type=MESH
        )
        return 0

    awaited = jnp.int32(nx - 1 + ny - 1)
    for side in CORNERS:
        there = exists(side)

        @pl.when(there)
        def _():
            pl.semaphore_signal(
                barrier, inc=1, device_id={"gx": gx + side[2], "gy": gy + side[3]}, device_id_type=MESH
            )

        awaited = awaited + jnp.where(there, 1, 0)
    lax.fori_loop(1, nx, greet, 0)
    lax.fori_loop(1, ny, greet_y, 0)

    for i in range(RBX):
        for j in range(RBY):
            live = counts[i, j]
            for s in range(1, SLOTS):
                code = codes[i, j, s]
                down = jnp.where(code >= 3, 1, 0) + jnp.where(code >= 6, 1, 0)
                row = (i + down) * 6 + j + code - 3 * down
                where[(i * RBY + j) * SLOTS + s] = jnp.where(s < live, row, ZERO_ROW)

    loads[0].wait()
    for i in range(RBX):
        for j in range(RBY):
            b = i * RBY + j
            row = guess[b : b + 1, :]
            sent[0, i, j] = row
            grid[(1 + i) * 6 + 1 + j] = row

    def transfer(step, side, source, target):
        index = SIDES.index(side)
        return pltpu.make_async_remote_copy(
            src_ref=source,
            dst_ref=target,
            send_sem=send_sems.at[step, index],
            recv_sem=recv_sems.at[step, index],
            device_id={"gx": gx - side[2], "gy": gy - side[3]},
            device_id_type=MESH,
        )

    def pieces(step, side):
        first, rows, dx, dy = side
        i = 1 if dx < 0 else 0
        j = RBY - 1 if dy < 0 else 0
        if dx and dy:
            return [transfer(step, side, sent.at[step, i, pl.ds(j, 1)], landed.at[step, pl.ds(first, 1)])]
        if dx:
            return [transfer(step, side, sent.at[step, i], landed.at[step, pl.ds(first, rows)])]
        return [
            transfer(step, side, sent.at[step, r, pl.ds(j, 1)], landed.at[step, pl.ds(first + r, 1)])
            for r in range(RBX)
        ]

    def whole(step, side):
        first, rows, _, _ = side
        part = landed.at[step, pl.ds(first, rows)]
        return transfer(step, side, part, part)

    def opposite(side):
        return (side[0], side[1], -side[2], -side[3])

    def send(step):
        for side in (*CORNERS, UP, DOWN, LEFT, RIGHT):

            @pl.when(exists(opposite(side)))
            def _():
                for piece in pieces(step, side):
                    piece.start()

    def receive(step, sides):
        for side in sides:

            @pl.when(exists(side))
            def _():
                whole(step, side).wait_recv()

        for side in sides:
            for row in range(side[0], side[0] + side[1]):
                r, c = GRID_OF[row]
                grid[r * 6 + c] = landed[step, row]

    def product(i, j):
        total = None
        for s in range(SLOTS):
            at = (1 + i) * 6 + 1 + j if s == 0 else where[(i * RBY + j) * SLOTS + s]
            term = tiles[i, j, s] * grid[at]
            total = term if total is None else total + term
        return jnp.sum(total.T, axis=0, keepdims=True)

    def advance(step, blocks):
        fresh = []
        for i, j in blocks:
            b = i * RBY + j
            image = product(i, j)
            if step == 0:
                new = right[b : b + 1, :] - image
            else:
                new = SCALE * (image - SHIFT * basis[step - 1, b : b + 1, :])
            fresh.append(new)
        for (i, j), new in zip(blocks, fresh):
            b = i * RBY + j
            basis[step, b : b + 1, :] = new
            if step < ITERS:
                sent[step + 1, i, j] = new

    def multiply_pairs(column):
        last = basis[column]
        for index, (i, j) in enumerate(PAIRS):
            if j == column:
                gram_rows[index : index + 1, :] = jnp.sum(basis[i] * last, axis=0, keepdims=True)

    gram_rows[len(PAIRS) : 16, :] = zero_line
    pl.semaphore_wait(barrier, awaited)
    send(0)
    loads[1].wait()
    for step in range(ITERS + 1):
        if step:
            multiply_pairs(step - 1)
            for i in range(RBX):
                for j in range(RBY):
                    grid[(1 + i) * 6 + 1 + j] = sent[step, i, j]
        for blocks, sides in ((order[:4], (UP, DOWN)), (order[4:], (LEFT, RIGHT, *CORNERS))):
            if step == 0:
                for at in blocks:
                    tile_loads[at].wait()
            receive(step, sides)
            advance(step, blocks)
        if step < ITERS:
            send(step + 1)
    multiply_pairs(ITERS)

    sublane = lax.broadcasted_iota(jnp.int32, (16, BLK), 0)
    lane = lax.broadcasted_iota(jnp.int32, (16, BLK), 1)
    own = sublane == lane

    total = jnp.sum(gram_rows[...], axis=1, keepdims=True)
    total = jnp.sum(jnp.where(own, jnp.broadcast_to(total, (16, BLK)), 0.0), axis=0, keepdims=True)
    for stage, (axis, n, here, sums) in enumerate((("gx", nx, gx, sums_x), ("gy", ny, gy, sums_y))):
        line[stage] = total
        sums[here] = total

        def copy_to(d):
            there = {"gx": gx, "gy": gy}
            there[axis] = lax.rem(here + d, n)
            return pltpu.make_async_remote_copy(
                src_ref=line.at[pl.ds(stage, 1)],
                dst_ref=sums.at[pl.ds(here, 1)],
                send_sem=sum_send_sems.at[stage],
                recv_sem=sum_recv_sems.at[stage],
                device_id=there,
                device_id_type=MESH,
            )

        for d in range(1, n):
            copy_to(d).start()
        others = sums.at[pl.ds(0, n - 1)]
        pltpu.make_async_remote_copy(
            src_ref=others,
            dst_ref=others,
            send_sem=sum_send_sems.at[stage],
            recv_sem=sum_recv_sems.at[stage],
            device_id={"gx": gx, "gy": gy},
            device_id_type=MESH,
        ).wait()
        parts = [sums[d] for d in range(n)]
        while len(parts) > 1:
            parts = [parts[k] + parts[k + 1] for k in range(0, len(parts), 2)]
        total = parts[0]
    spread = jnp.sum(
        jnp.where(own, jnp.broadcast_to(total, (16, BLK)), 0.0), axis=1, keepdims=True
    )
    gram[...] = jnp.broadcast_to(spread, (16, BLK))
    g = {}
    for index, (i, j) in enumerate(PAIRS):
        g[i, j] = jnp.broadcast_to(gram[index : index + 1, :], (ROWS, BLK))

    def factor(m, n):
        r, inverse = {}, []
        m = dict(m)
        for k in range(n):
            root = jnp.sqrt(m[k, k])
            r[k, k] = root
            inverse.append(1.0 / root)
            for j in range(k + 1, n):
                r[k, j] = m[k, j] * inverse[k]
            for i in range(k + 1, n):
                for j in range(i, n):
                    m[i, j] = m[i, j] - r[k, i] * r[k, j]
        return r, inverse

    r, inverse = factor(g, ITERS + 1)
    h = {}
    for k in range(ITERS):
        for i in range(k + 2):
            value = r[i, k + 1]
            for m in range(max(i - 1, 0), k):
                value = value - h[i, m] * r[m, k]
            h[i, k] = value * inverse[k]
    for i, k in h:
        h[i, k] = h[i, k] * (1.0 / SCALE)
        if i == k:
            h[i, k] = h[i, k] + SHIFT
    normal = {}
    for i in range(ITERS):
        for j in range(i, ITERS):
            value = None
            for k in range(i + 2):
                term = h[k, i] * h[k, j]
                value = term if value is None else value + term
            normal[i, j] = value
    target = [r[0, 0] * h[0, k] for k in range(ITERS)]
    lower, scale = factor(normal, ITERS)

    def substitute_back(upper, reciprocal, values):
        found = [None] * ITERS
        for row in reversed(range(ITERS)):
            value = values[row]
            for column in range(row + 1, ITERS):
                value = value - upper[row, column] * found[column]
            found[row] = value * reciprocal[row]
        return found

    forward = []
    for row in range(ITERS):
        value = target[row]
        for column in range(row):
            value = value - lower[column, row] * forward[column]
        forward.append(value * scale[row])
    y = substitute_back(lower, scale, forward)
    weights = substitute_back(r, inverse, y)

    found = guess[...]
    left = basis[0]
    for k in range(ITERS):
        found = found + weights[k] * basis[k]
        left = left - weights[k] * ((1.0 / SCALE) * basis[k + 1] + SHIFT * basis[k])
    solution_ref[...] = found
    residual_ref[...] = left
    sublane, lane = sublane[:ROWS], lane[:ROWS]
    shown = jnp.zeros((ROWS, BLK), jnp.float32)
    for i, k in h:
        shown = jnp.where(jnp.logical_and(sublane == i, lane == k), h[i, k], shown)
    hessenberg_ref[...] = shown[: ITERS + 1, :ITERS]

    for step in range(ITERS + 1):
        for side in SIDES:

            @pl.when(exists(opposite(side)))
            def _():
                whole(step, side).wait_send()


def solution(mesh):
    nx, ny = mesh.shape["gx"], mesh.shape["gy"]

    def body(matrix_tiles, tile_codes, tile_counts, right_side, initial_guess):
        flat = jax.ShapeDtypeStruct((ROWS, BLK), jnp.float32)
        any_space = pl.BlockSpec(memory_space=pl.ANY)
        vmem = pl.BlockSpec(memory_space=pltpu.VMEM)
        smem = pl.BlockSpec(memory_space=pltpu.SMEM)
        found, left, hessenberg = pl.pallas_call(
            functools.partial(kernel, nx, ny),
            out_shape=(flat, flat, jax.ShapeDtypeStruct((ITERS + 1, ITERS), jnp.float32)),
            in_specs=[any_space, smem, smem, any_space, any_space],
            out_specs=(vmem, vmem, vmem),
            scratch_shapes=[
                pltpu.VMEM((RBX, RBY, SLOTS, BLK, BLK), jnp.float32),
                pltpu.VMEM((ZERO_ROW + 1, 1, BLK), jnp.float32),
                pltpu.SMEM((ROWS * SLOTS,), jnp.int32),
                pltpu.VMEM((ITERS + 1, RBX, RBY, 1, BLK), jnp.float32),
                pltpu.VMEM((ITERS + 1, 16, 1, BLK), jnp.float32),
                pltpu.VMEM((ITERS + 1, ROWS, BLK), jnp.float32),
                pltpu.VMEM((ROWS, BLK), jnp.float32),
                pltpu.VMEM((ROWS, BLK), jnp.float32),
                pltpu.VMEM((16, BLK), jnp.float32),
                pltpu.VMEM((16, BLK), jnp.float32),
                pltpu.VMEM((2, 1, BLK), jnp.float32),
                pltpu.VMEM((nx, 1, BLK), jnp.float32),
                pltpu.VMEM((ny, 1, BLK), jnp.float32),
                pltpu.SemaphoreType.DMA((ROWS,)),
                pltpu.SemaphoreType.DMA((2,)),
                pltpu.SemaphoreType.DMA((ITERS + 1, len(SIDES))),
                pltpu.SemaphoreType.DMA((ITERS + 1, len(SIDES))),
                pltpu.SemaphoreType.DMA((2,)),
                pltpu.SemaphoreType.DMA((2,)),
            ],
            compiler_params=pltpu.CompilerParams(collective_id=0, has_side_effects=True),
        )(
            matrix_tiles,
            tile_codes,
            tile_counts,
            right_side.reshape(ROWS, BLK),
            initial_guess.reshape(ROWS, BLK),
        )
        shape = (RBX, RBY, BLK)
        return found.reshape(shape), left.reshape(shape), hessenberg

    split = P("gx", "gy", None)
    return jax.shard_map(
        body,
        mesh=mesh,
        in_specs=(P("gx", "gy", None, None, None), split, P("gx", "gy"), split, split),
        out_specs=(split, split, P()),
        check_vma=False,
    )
```

```python
import functools

import jax
import jax.numpy as jnp
from jax import lax
from jax.experimental import pallas as pl
from jax.experimental.pallas import tpu as pltpu
from jax.sharding import PartitionSpec as P

ITERS = 4
SLOTS = 6
BLK = 128
RBX = 2
RBY = 4
ROWS = RBX * RBY
SHIFT = 3.0
SCALE = 0.25
PAIRS = [(i, j) for j in range(ITERS + 1) for i in range(j + 1)]
MESH = pl.DeviceIdType.MESH

UP, DOWN, LEFT, RIGHT = (0, 4, -1, 0), (4, 4, 1, 0), (8, 2, 0, -1), (10, 2, 0, 1)
CORNERS = ((12, 1, -1, -1), (13, 1, -1, 1), (14, 1, 1, -1), (15, 1, 1, 1))
SIDES = (UP, DOWN, LEFT, RIGHT, *CORNERS)
GRID_OF = (
    [(0, 1 + j) for j in range(RBY)]
    + [(3, 1 + j) for j in range(RBY)]
    + [(1 + i, 0) for i in range(RBX)]
    + [(1 + i, 5) for i in range(RBX)]
    + [(0, 0), (0, 5), (3, 0), (3, 5)]
)
ZERO_ROW = 24
VMEM_BYTES = 67043328


def kernel(
    nx, ny,
    tiles_hbm, codes_hbm, counts_hbm, right_hbm, guess_hbm,
    basis, guess, gram,
    tiles, grid, codes, counts, where, sent, landed, right,
    gram_rows, line, sums_x, sums_y,
    tile_sems, load_sems, send_sems, recv_sems, sum_send_sems, sum_recv_sems,
):
    gx, gy = lax.axis_index("gx"), lax.axis_index("gy")

    zero_line = jnp.zeros((1, BLK), jnp.float32)
    for step in range(ITERS + 1):
        for row in range(16):
            landed[step, row] = zero_line
    grid[ZERO_ROW] = zero_line

    def exists(side):
        _, _, dx, dy = side
        ok = None
        for at, d, n in ((gx, dx, nx), (gy, dy, ny)):
            if d:
                here = at > 0 if d < 0 else at < n - 1
                ok = here if ok is None else jnp.logical_and(ok, here)
        return ok

    barrier = pltpu.get_barrier_semaphore()

    def greet(d, _):
        pl.semaphore_signal(
            barrier, inc=1, device_id={"gx": lax.rem(gx + d, nx), "gy": gy}, device_id_type=MESH
        )
        return 0

    def greet_y(d, _):
        pl.semaphore_signal(
            barrier, inc=1, device_id={"gx": gx, "gy": lax.rem(gy + d, ny)}, device_id_type=MESH
        )
        return 0

    awaited = jnp.int32(nx - 1 + ny - 1)
    for side in CORNERS:
        there = exists(side)

        @pl.when(there)
        def _():
            pl.semaphore_signal(
                barrier, inc=1, device_id={"gx": gx + side[2], "gy": gy + side[3]}, device_id_type=MESH
            )

        awaited = awaited + jnp.where(there, 1, 0)
    lax.fori_loop(1, nx, greet, 0)
    lax.fori_loop(1, ny, greet_y, 0)

    loads = [
        pltpu.make_async_copy(guess_hbm, guess, load_sems.at[0]),
        pltpu.make_async_copy(right_hbm, right, load_sems.at[1]),
        pltpu.make_async_copy(codes_hbm, codes, load_sems.at[2]),
        pltpu.make_async_copy(counts_hbm, counts, load_sems.at[3]),
    ]
    for load in loads:
        load.start()
    order = [(i, j) for j in (1, 2) for i in (0, 1)] + [(i, j) for j in (0, 3) for i in (0, 1)]
    tile_loads = {
        (i, j): pltpu.make_async_copy(tiles_hbm.at[i, j], tiles.at[i, j], tile_sems.at[i * RBY + j])
        for i, j in order
    }
    for at in order:
        tile_loads[at].start()

    loads[0].wait()
    for i in range(RBX):
        for j in range(RBY):
            b = i * RBY + j
            row = guess[b : b + 1, :]
            sent[0, i, j] = row
            grid[(1 + i) * 6 + 1 + j] = row

    def transfer(step, side, source, target):
        index = SIDES.index(side)
        return pltpu.make_async_remote_copy(
            src_ref=source,
            dst_ref=target,
            send_sem=send_sems.at[step, index],
            recv_sem=recv_sems.at[step, index],
            device_id={"gx": gx - side[2], "gy": gy - side[3]},
            device_id_type=MESH,
        )

    def pieces(step, side):
        first, rows, dx, dy = side
        i = 1 if dx < 0 else 0
        j = RBY - 1 if dy < 0 else 0
        if dx and dy:
            return [transfer(step, side, sent.at[step, i, pl.ds(j, 1)], landed.at[step, pl.ds(first, 1)])]
        if dx:
            return [transfer(step, side, sent.at[step, i], landed.at[step, pl.ds(first, rows)])]
        return [
            transfer(step, side, sent.at[step, r, pl.ds(j, 1)], landed.at[step, pl.ds(first + r, 1)])
            for r in range(RBX)
        ]

    def whole(step, side):
        first, rows, _, _ = side
        part = landed.at[step, pl.ds(first, rows)]
        return transfer(step, side, part, part)

    def opposite(side):
        return (side[0], side[1], -side[2], -side[3])

    def send(step):
        for side in (*CORNERS, UP, DOWN, LEFT, RIGHT):

            @pl.when(exists(opposite(side)))
            def _():
                for piece in pieces(step, side):
                    piece.start()

    def receive(step, sides):
        for side in sides:

            @pl.when(exists(side))
            def _():
                whole(step, side).wait_recv()

        for side in sides:
            for row in range(side[0], side[0] + side[1]):
                r, c = GRID_OF[row]
                grid[r * 6 + c] = landed[step, row]

    def product(i, j):
        total = None
        for s in range(SLOTS):
            at = (1 + i) * 6 + 1 + j if s == 0 else where[(i * RBY + j) * SLOTS + s]
            term = tiles[i, j, s] * grid[at]
            total = term if total is None else total + term
        return jnp.sum(total.T, axis=0, keepdims=True)

    def advance(step, blocks):
        fresh = []
        for i, j in blocks:
            b = i * RBY + j
            image = product(i, j)
            if step == 0:
                new = right[b : b + 1, :] - image
            else:
                new = SCALE * (image - SHIFT * basis[step - 1, b : b + 1, :])
            fresh.append(new)
        for (i, j), new in zip(blocks, fresh):
            b = i * RBY + j
            basis[step, b : b + 1, :] = new
            if step < ITERS:
                sent[step + 1, i, j] = new

    def multiply_pairs(column):
        last = basis[column]
        for index, (i, j) in enumerate(PAIRS):
            if j == column:
                gram_rows[index : index + 1, :] = jnp.sum(basis[i] * last, axis=0, keepdims=True)

    gram_rows[len(PAIRS) : 16, :] = zero_line
    pl.semaphore_wait(barrier, awaited)
    send(0)
    loads[2].wait()
    loads[3].wait()
    for i in range(RBX):
        for j in range(RBY):
            live = counts[i, j]
            for s in range(1, SLOTS):
                code = codes[i, j, s]
                down = jnp.where(code >= 3, 1, 0) + jnp.where(code >= 6, 1, 0)
                row = (i + down) * 6 + j + code - 3 * down
                where[(i * RBY + j) * SLOTS + s] = jnp.where(s < live, row, ZERO_ROW)

    loads[1].wait()
    for step in range(ITERS + 1):
        if step:
            multiply_pairs(step - 1)
            for i in range(RBX):
                for j in range(RBY):
                    grid[(1 + i) * 6 + 1 + j] = sent[step, i, j]
        for blocks, sides in ((order[:4], (UP, DOWN)), (order[4:], (LEFT, RIGHT, *CORNERS))):
            if step == 0:
                for at in blocks:
                    tile_loads[at].wait()
            receive(step, sides)
            advance(step, blocks)
        if step < ITERS:
            send(step + 1)
    multiply_pairs(ITERS)

    sublane = lax.broadcasted_iota(jnp.int32, (16, BLK), 0)
    lane = lax.broadcasted_iota(jnp.int32, (16, BLK), 1)
    own = sublane == lane

    total = jnp.sum(gram_rows[...], axis=1, keepdims=True)
    total = jnp.sum(jnp.where(own, jnp.broadcast_to(total, (16, BLK)), 0.0), axis=0, keepdims=True)
    for stage, (axis, n, here, sums) in enumerate((("gx", nx, gx, sums_x), ("gy", ny, gy, sums_y))):
        line[stage] = total
        sums[here] = total

        def copy_to(d):
            there = {"gx": gx, "gy": gy}
            there[axis] = lax.rem(here + d, n)
            return pltpu.make_async_remote_copy(
                src_ref=line.at[pl.ds(stage, 1)],
                dst_ref=sums.at[pl.ds(here, 1)],
                send_sem=sum_send_sems.at[stage],
                recv_sem=sum_recv_sems.at[stage],
                device_id=there,
                device_id_type=MESH,
            )

        for d in range(1, n):
            copy_to(d).start()
        others = sums.at[pl.ds(0, n - 1)]
        pltpu.make_async_remote_copy(
            src_ref=others,
            dst_ref=others,
            send_sem=sum_send_sems.at[stage],
            recv_sem=sum_recv_sems.at[stage],
            device_id={"gx": gx, "gy": gy},
            device_id_type=MESH,
        ).wait()
        parts = [sums[d] for d in range(n)]
        while len(parts) > 1:
            parts = [parts[k] + parts[k + 1] for k in range(0, len(parts), 2)]
        total = parts[0]
    gram[...] = total

    for step in range(ITERS + 1):
        for side in SIDES:

            @pl.when(exists(opposite(side)))
            def _():
                whole(step, side).wait_send()


def finish(basis, guess, gram, solution_ref, residual_ref, hessenberg_ref, entries):
    sublane = lax.broadcasted_iota(jnp.int32, (16, BLK), 0)
    lane = lax.broadcasted_iota(jnp.int32, (16, BLK), 1)
    own = sublane == lane
    spread = jnp.sum(
        jnp.where(own, jnp.broadcast_to(gram[...], (16, BLK)), 0.0), axis=1, keepdims=True
    )
    entries[...] = jnp.broadcast_to(spread, (16, BLK))
    g = {}
    for index, (i, j) in enumerate(PAIRS):
        g[i, j] = jnp.broadcast_to(entries[index : index + 1, :], (ROWS, BLK))

    def factor(m, n):
        r, inverse = {}, []
        m = dict(m)
        for k in range(n):
            root = jnp.sqrt(m[k, k])
            r[k, k] = root
            inverse.append(1.0 / root)
            for j in range(k + 1, n):
                r[k, j] = m[k, j] * inverse[k]
            for i in range(k + 1, n):
                for j in range(i, n):
                    m[i, j] = m[i, j] - r[k, i] * r[k, j]
        return r, inverse

    r, inverse = factor(g, ITERS + 1)
    h = {}
    for k in range(ITERS):
        for i in range(k + 2):
            value = r[i, k + 1]
            for m in range(max(i - 1, 0), k):
                value = value - h[i, m] * r[m, k]
            h[i, k] = value * inverse[k]
    for i, k in h:
        h[i, k] = h[i, k] * (1.0 / SCALE)
        if i == k:
            h[i, k] = h[i, k] + SHIFT
    normal = {}
    for i in range(ITERS):
        for j in range(i, ITERS):
            value = None
            for k in range(i + 2):
                term = h[k, i] * h[k, j]
                value = term if value is None else value + term
            normal[i, j] = value
    target = [r[0, 0] * h[0, k] for k in range(ITERS)]
    lower, scale = factor(normal, ITERS)

    def substitute_back(upper, reciprocal, values):
        found = [None] * ITERS
        for row in reversed(range(ITERS)):
            value = values[row]
            for column in range(row + 1, ITERS):
                value = value - upper[row, column] * found[column]
            found[row] = value * reciprocal[row]
        return found

    forward = []
    for row in range(ITERS):
        value = target[row]
        for column in range(row):
            value = value - lower[column, row] * forward[column]
        forward.append(value * scale[row])
    y = substitute_back(lower, scale, forward)
    weights = substitute_back(r, inverse, y)

    found = guess[...]
    left = basis[0]
    for k in range(ITERS):
        found = found + weights[k] * basis[k]
        left = left - weights[k] * ((1.0 / SCALE) * basis[k + 1] + SHIFT * basis[k])
    solution_ref[...] = found
    residual_ref[...] = left
    sublane, lane = sublane[:ROWS], lane[:ROWS]
    shown = jnp.zeros((ROWS, BLK), jnp.float32)
    for i, k in h:
        shown = jnp.where(jnp.logical_and(sublane == k, lane == i), h[i, k], shown)
    hessenberg_ref[...] = shown[:ITERS, : ITERS + 1]


def solution(mesh):
    nx, ny = mesh.shape["gx"], mesh.shape["gy"]

    def body(matrix_tiles, tile_codes, tile_counts, right_side, initial_guess):
        flat = jax.ShapeDtypeStruct((ROWS, BLK), jnp.float32)
        hbm = pl.BlockSpec(memory_space=pltpu.HBM)
        vmem = pl.BlockSpec(memory_space=pltpu.VMEM)
        parts = pl.pallas_call(
            functools.partial(kernel, nx, ny),
            out_shape=(
                pltpu.VMEM((ITERS + 1, ROWS, BLK), jnp.float32),
                pltpu.VMEM((ROWS, BLK), jnp.float32),
                pltpu.VMEM((1, BLK), jnp.float32),
            ),
            in_specs=[hbm] * 5,
            out_specs=(vmem, vmem, vmem),
            scratch_shapes=[
                pltpu.VMEM((RBX, RBY, SLOTS, BLK, BLK), jnp.float32),
                pltpu.VMEM((ZERO_ROW + 1, 1, BLK), jnp.float32),
                pltpu.SMEM((RBX, RBY, SLOTS), jnp.int32),
                pltpu.SMEM((RBX, RBY), jnp.int32),
                pltpu.SMEM((ROWS * SLOTS,), jnp.int32),
                pltpu.VMEM((ITERS + 1, RBX, RBY, 1, BLK), jnp.float32),
                pltpu.VMEM((ITERS + 1, 16, 1, BLK), jnp.float32),
                pltpu.VMEM((ROWS, BLK), jnp.float32),
                pltpu.VMEM((16, BLK), jnp.float32),
                pltpu.VMEM((2, 1, BLK), jnp.float32),
                pltpu.VMEM((nx, 1, BLK), jnp.float32),
                pltpu.VMEM((ny, 1, BLK), jnp.float32),
                pltpu.SemaphoreType.DMA((ROWS,)),
                pltpu.SemaphoreType.DMA((4,)),
                pltpu.SemaphoreType.DMA((ITERS + 1, len(SIDES))),
                pltpu.SemaphoreType.DMA((ITERS + 1, len(SIDES))),
                pltpu.SemaphoreType.DMA((2,)),
                pltpu.SemaphoreType.DMA((2,)),
            ],
            compiler_params=pltpu.CompilerParams(
                collective_id=0, has_side_effects=True, vmem_limit_bytes=VMEM_BYTES - 40960
            ),
        )(
            matrix_tiles,
            tile_codes,
            tile_counts,
            right_side.reshape(ROWS, BLK),
            initial_guess.reshape(ROWS, BLK),
        )
        found, left, hessenberg = pl.pallas_call(
            finish,
            out_shape=(flat, flat, jax.ShapeDtypeStruct((ITERS, ITERS + 1), jnp.float32)),
            in_specs=[vmem] * 3,
            out_specs=(vmem, vmem, vmem),
            scratch_shapes=[pltpu.VMEM((16, BLK), jnp.float32)],
            compiler_params=pltpu.CompilerParams(vmem_limit_bytes=1 << 20),
        )(*parts)
        shape = (RBX, RBY, BLK)
        return found.reshape(shape), left.reshape(shape), hessenberg.T

    split = P("gx", "gy", None)
    return jax.shard_map(
        body,
        mesh=mesh,
        in_specs=(P("gx", "gy", None, None, None), split, P("gx", "gy"), split, split),
        out_specs=(split, split, P()),
        check_vma=False,
    )
```
